32 devices in a mesh: grp: 2 (over x), dap: 16 (over z, y, core).
Axes of the slice: x: 2, y: 2, z: 4, core: 2. Of those that a mesh axis runs over, the one named last changes fastest.
Arguments:
- homolog_stack_tensor: bfloat16 [64, 64, 256], P(('grp', 'dap')), parts along dimension 0, may hold values from -6.5 to 6.5
- occupancy_indicator: int32 [64, 64], P('grp'), parts along dimension 0, may hold values from 0 to 1, as said below
- chain_existence_flags: int32 [64], P('grp'), parts along dimension 0, may hold values from 0 to 1, as said below
- focus_normal_factor: float32 [256], replicated, may hold values from 0.25 to 1.75
- focus_normal_addend: float32 [256], replicated, may hold values from -3 to 3
- probe_index_weights: bfloat16 [256, 512], replicated, may hold values from -3 to 3
- payload_valve_weights: bfloat16 [256, 512], replicated, may hold values from -0.375 to 0.375
- logistic_valve_addend: float32 [256], replicated, may hold values from -4 to 4
- focus_exit_weights: bfloat16 [256, 256], replicated, may hold values from -0.375 to 0.375
- focus_exit_addend: float32 [256], replicated, may hold values from -3 to 3
- product_mean_layer_stretch: float32 [256], replicated, may hold values from 0.25 to 1.75
- product_mean_layer_shift: float32 [256], replicated, may hold values from -2 to 2
- twin_map_matrix: bfloat16 [256, 64], replicated, may hold values from -0.375 to 0.375
- twin_map_shift: float32 [64], replicated, may hold values from -2 to 2
- couple_map_matrix: bfloat16 [1024, 128], replicated, may hold values from -0.75 to 0.75
- couple_map_shift: float32 [128], replicated, may hold values from -3 to 3
Outputs:
- alignment_after: bfloat16 [64, 64, 256], P('grp', 'dap'), parts along dimension 0
- pair_features_after: bfloat16 [128, 64, 128], P(('grp', 'dap')), parts along dimension 0
The draws below stay inside these ranges and needn't reach their ends.
There are 2 independent parts, one for each index of `grp`. The reference program is written for one: setup_inputs(seed, part) draws one part's arguments, and reference() takes and returns one part's arrays. A program takes and returns all parts, laid end to end along the dimension named above; an argument that names none is the same for every part. Nothing has to cross between parts.
Inputs may be any that keep to these rules, and one draw needn't show every extreme that they name: `chain_existence_flags`: 1 for the first 16 sequences, 0 for the last one. `occupancy_indicator`: every sequence is 0 from some residue on (the last residue always, never more than the last 32); before it sequence 0 is all 1 and the others have gaps.
All inputs are finite; a program needn't handle non-finite values.
Results may differ from the reference program's by a relative error of at most 0.008.
Values may be sent and summed in bfloat16 or wider, within the bound.
No kernel may reach another device: no remote copies, remote signals or barrier semaphores. Data moves between devices by JAX's collectives and lax.ppermute only.
A program may use at most 64 MiB of HBM per device.

```python
import jax
import jax.numpy as jnp
from jax import lax

ALIGN_CHANNELS = 256
HEAD_COUNT = 8
HEAD_CHANNELS = 32
OUTER_CHANNELS = 32
PAIR_DIM = 128
SITES_EACH_SLICE = 4
SEQUENCE_COUNT = 32
RESIDUE_COUNT = 64


def draw_homolog_stack_tensor(key, part):
    random_root_key = jax.random.fold_in(jax.random.fold_in(key, 101), 0)
    value_vectors = jax.random.normal(random_root_key, (SEQUENCE_COUNT, RESIDUE_COUNT, ALIGN_CHANNELS), jnp.float32)
    return jnp.clip(value_vectors, -6.5, 6.5).astype(jnp.bfloat16)


def draw_probe_index_weights(key, part):
    query_seed_value, second_seed_value = jax.random.split(jax.random.fold_in(key, 202))
    inner_channel_width = HEAD_COUNT * HEAD_CHANNELS
    square_root_width = jnp.sqrt(jnp.float32(ALIGN_CHANNELS))
    query_rows_all = jnp.clip(jax.random.normal(query_seed_value, (ALIGN_CHANNELS, inner_channel_width), jnp.float32), -6.0, 6.0) / square_root_width
    key_portion = jnp.clip(jax.random.normal(second_seed_value, (ALIGN_CHANNELS, inner_channel_width), jnp.float32), -6.0, 6.0) / square_root_width
    combined = jnp.concatenate([query_rows_all, key_portion], axis=1)
    return jnp.clip(combined, -3.0, 3.0).astype(jnp.bfloat16)


def draw_chain_existence_flags(key, part):
    coin_flips = jax.random.randint(jax.random.fold_in(key, 303), (SEQUENCE_COUNT,), 0, 2)
    position = jnp.arange(SEQUENCE_COUNT, dtype=jnp.int32)
    forced_on = position < SEQUENCE_COUNT // 2
    forced_off = position == SEQUENCE_COUNT - 1
    return jnp.where(forced_on, 1, jnp.where(forced_off, 0, coin_flips)).astype(jnp.int32)


def draw_occupancy_indicator(key, part):
    length_key, gap_key = jax.random.split(jax.random.fold_in(key, 404))
    length = jax.random.randint(length_key, (), RESIDUE_COUNT // 2, RESIDUE_COUNT)
    gap_draw = jax.random.randint(gap_key, (SEQUENCE_COUNT, RESIDUE_COUNT), 0, 8)
    inside = jnp.arange(RESIDUE_COUNT, dtype=jnp.int32)[None, :] < length
    first_row = jnp.arange(SEQUENCE_COUNT, dtype=jnp.int32)[:, None] == 0
    return (inside & ((gap_draw != 0) | first_row)).astype(jnp.int32)


def gaussian(own_key, shape, scale, limit, kind=jnp.bfloat16):
    entries = jax.random.normal(own_key, shape, jnp.float32) * scale
    return jnp.minimum(jnp.maximum(entries, -limit), limit).astype(kind)


def setup_inputs(seed: int = 0, part: int = 0) -> dict:
    key_list = jax.random.split(jax.random.key(seed), 17)
    part_keys = jax.random.split(jax.random.fold_in(key_list[16], part), 17)
    return {
        "homolog_stack_tensor": draw_homolog_stack_tensor(jax.random.fold_in(jax.random.fold_in(key_list[16], part), 71), part),
        "occupancy_indicator": draw_occupancy_indicator(jax.random.fold_in(jax.random.fold_in(key_list[16], part), 71), part),
        "chain_existence_flags": draw_chain_existence_flags(jax.random.fold_in(jax.random.fold_in(key_list[16], part), 71), part),
        "focus_normal_factor": jnp.clip(1.0 + 0.15 * jax.random.normal(key_list[3], (ALIGN_CHANNELS,), jnp.float32), 0.25, 1.75),
        "focus_normal_addend": gaussian(key_list[4], (ALIGN_CHANNELS,), 0.5, 3.0, jnp.float32),
        "probe_index_weights": draw_probe_index_weights(jax.random.fold_in(key_list[16], 71), part),
        "payload_valve_weights": gaussian(key_list[6], (ALIGN_CHANNELS, 2 * HEAD_COUNT * HEAD_CHANNELS), ALIGN_CHANNELS ** -0.5, 0.375),
        "logistic_valve_addend": gaussian(key_list[7], (HEAD_COUNT * HEAD_CHANNELS,), 1.0, 4.0, jnp.float32),
        "focus_exit_weights": gaussian(key_list[8], (HEAD_COUNT * HEAD_CHANNELS, ALIGN_CHANNELS), (HEAD_COUNT * HEAD_CHANNELS) ** -0.5, 0.375),
        "focus_exit_addend": gaussian(key_list[9], (ALIGN_CHANNELS,), 0.5, 3.0, jnp.float32),
        "product_mean_layer_stretch": jnp.clip(1.0 + 0.15 * jax.random.normal(key_list[10], (ALIGN_CHANNELS,), jnp.float32), 0.25, 1.75),
        "product_mean_layer_shift": gaussian(key_list[11], (ALIGN_CHANNELS,), 0.3, 2.0, jnp.float32),
        "twin_map_matrix": gaussian(key_list[12], (ALIGN_CHANNELS, 2 * OUTER_CHANNELS), ALIGN_CHANNELS ** -0.5, 0.375),
        "twin_map_shift": gaussian(key_list[13], (2 * OUTER_CHANNELS,), 0.3, 2.0, jnp.float32),
        "couple_map_matrix": gaussian(key_list[14], (OUTER_CHANNELS * OUTER_CHANNELS, PAIR_DIM), (OUTER_CHANNELS * OUTER_CHANNELS // 16) ** -0.5, 0.75),
        "couple_map_shift": gaussian(key_list[15], (PAIR_DIM,), 0.5, 3.0, jnp.float32),
    }


EPSILON = 1e-05
MASKED = -100000.0

def layer_norm(value_vectors, scale_vec, shift_vec):
    widened = value_vectors.astype(jnp.float32)
    centred = widened - lax.optimization_barrier(jnp.mean(widened, axis=-1, keepdims=True))
    variance = lax.optimization_barrier(jnp.mean(centred * centred, axis=-1, keepdims=True))
    scaled = centred * lax.rsqrt(variance + EPSILON)
    return (scaled * scale_vec.astype(jnp.float32) + shift_vec.astype(jnp.float32)).astype(jnp.bfloat16)

def heed_across_lanes(vertical_pieces, present_mask, focus_normal_factor, focus_normal_addend, probe_index_weights, payload_valve_weights, logistic_valve_addend, focus_exit_weights, focus_exit_addend):
    seq_count, res_count, feature_width = vertical_pieces.shape
    inner_channel_width = HEAD_COUNT * HEAD_CHANNELS
    normed = layer_norm(vertical_pieces, focus_normal_factor, focus_normal_addend).reshape(seq_count * res_count, feature_width)
    query_key = jnp.dot(normed, probe_index_weights, preferred_element_type=jnp.float32)
    value_gate = jnp.dot(normed, payload_valve_weights, preferred_element_type=jnp.float32)
    head_shape = (seq_count, res_count, HEAD_COUNT, HEAD_CHANNELS)
    query_rows_all = (query_key[:, :inner_channel_width] * HEAD_CHANNELS ** (-0.5)).astype(jnp.bfloat16).reshape(head_shape)
    key_rows = query_key[:, inner_channel_width:].astype(jnp.bfloat16).reshape(head_shape)
    value_rows = value_gate[:, :inner_channel_width].astype(jnp.bfloat16).reshape(head_shape)
    gating = jax.nn.sigmoid(value_gate[:, inner_channel_width:] + logistic_valve_addend.astype(jnp.float32))
    scores = jnp.einsum('srhd,trhd->rhst', query_rows_all.astype(jnp.float32), key_rows.astype(jnp.float32))
    allowed = jnp.transpose(present_mask > 0)[:, None, None, :]
    scores = jnp.where(allowed, scores, MASKED)
    exponent = jnp.exp(scores - lax.optimization_barrier(jnp.max(scores, axis=-1, keepdims=True)))
    weights = (exponent / lax.optimization_barrier(jnp.sum(exponent, axis=-1, keepdims=True))).astype(jnp.bfloat16)
    attended = jnp.einsum('rhst,trhd->srhd', weights.astype(jnp.float32), value_rows.astype(jnp.float32))
    gated_rows = (attended.reshape(seq_count * res_count, inner_channel_width) * gating).astype(jnp.bfloat16)
    update = jnp.dot(gated_rows, focus_exit_weights, preferred_element_type=jnp.float32) + focus_exit_addend.astype(jnp.float32)
    return (vertical_pieces.astype(jnp.float32) + update.reshape(seq_count, res_count, feature_width)).astype(jnp.bfloat16)

def project_pairs(revised_tensor, present_mask, product_mean_layer_stretch, product_mean_layer_shift, twin_map_matrix, twin_map_shift):
    seq_count, res_count, feature_width = revised_tensor.shape
    normed = layer_norm(revised_tensor, product_mean_layer_stretch, product_mean_layer_shift).reshape(seq_count * res_count, feature_width)
    projected = jnp.dot(normed, twin_map_matrix, preferred_element_type=jnp.float32) + twin_map_shift.astype(jnp.float32)
    projected = projected.reshape(seq_count, res_count, 2 * OUTER_CHANNELS) * present_mask[:, :, None].astype(jnp.float32)
    projected = projected.astype(jnp.bfloat16)
    return (projected[:, :, :OUTER_CHANNELS], projected[:, :, OUTER_CHANNELS:])

def pair_tile(left_rows, right_cols, live_rows, live_cols, couple_map_matrix, couple_map_shift):
    row_count = left_rows.shape[1]
    col_count = right_cols.shape[1]
    outer_sum = jnp.einsum('sic,sje->ijce', left_rows.astype(jnp.float32), right_cols.astype(jnp.float32))
    counts = jnp.einsum('si,sj->ij', live_rows.astype(jnp.float32), live_cols.astype(jnp.float32))
    mean_terms = (outer_sum.reshape(row_count, col_count, OUTER_CHANNELS * OUTER_CHANNELS) / jnp.maximum(counts, 1.0)[:, :, None]).astype(jnp.bfloat16)
    result = jnp.dot(mean_terms.reshape(row_count * col_count, OUTER_CHANNELS * OUTER_CHANNELS), couple_map_matrix, preferred_element_type=jnp.float32)
    result = result + couple_map_shift.astype(jnp.float32)
    return result.astype(jnp.bfloat16).reshape(row_count, col_count, PAIR_DIM)

def reference(homolog_stack_tensor, occupancy_indicator, chain_existence_flags, focus_normal_factor, focus_normal_addend, probe_index_weights, payload_valve_weights, logistic_valve_addend, focus_exit_weights, focus_exit_addend, product_mean_layer_stretch, product_mean_layer_shift, twin_map_matrix, twin_map_shift, couple_map_matrix, couple_map_shift):
    present_mask = occupancy_indicator * chain_existence_flags[:, None]
    block_count = RESIDUE_COUNT // SITES_EACH_SLICE

    def column_block(block_index):
        opening_index = (block_index * SITES_EACH_SLICE).astype(jnp.int32)
        homolog_owned_block = lax.dynamic_slice_in_dim(homolog_stack_tensor, opening_index, SITES_EACH_SLICE, 1)
        current_fraction = lax.dynamic_slice_in_dim(present_mask, opening_index, SITES_EACH_SLICE, 1)
        revised_tensor = heed_across_lanes(homolog_owned_block, current_fraction, focus_normal_factor, focus_normal_addend, probe_index_weights, payload_valve_weights, logistic_valve_addend, focus_exit_weights, focus_exit_addend)
        left_part, right_part = project_pairs(revised_tensor, current_fraction, product_mean_layer_stretch, product_mean_layer_shift, twin_map_matrix, twin_map_shift)
        return (revised_tensor, left_part, right_part)
    refreshed_blocks, left_blocks, right_blocks = lax.map(column_block, jnp.arange(block_count, dtype=jnp.int32))
    alignment_after = jnp.transpose(refreshed_blocks, (1, 0, 2, 3)).reshape(SEQUENCE_COUNT, RESIDUE_COUNT, ALIGN_CHANNELS)
    left_all = jnp.transpose(left_blocks, (1, 0, 2, 3)).reshape(SEQUENCE_COUNT, RESIDUE_COUNT, OUTER_CHANNELS)
    right_all = jnp.transpose(right_blocks, (1, 0, 2, 3)).reshape(SEQUENCE_COUNT, RESIDUE_COUNT, OUTER_CHANNELS)

    def pair_block(block_index):
        opening_index = (block_index * SITES_EACH_SLICE).astype(jnp.int32)
        rows_left = lax.dynamic_slice_in_dim(left_all, opening_index, SITES_EACH_SLICE, 1)
        rows_live = lax.dynamic_slice_in_dim(present_mask, opening_index, SITES_EACH_SLICE, 1)
        return pair_tile(rows_left, right_all, rows_live, present_mask, couple_map_matrix, couple_map_shift)
    pair_blocks = lax.map(pair_block, jnp.arange(block_count, dtype=jnp.int32))
    pair_features_after = pair_blocks.reshape(RESIDUE_COUNT, RESIDUE_COUNT, PAIR_DIM)
    return (alignment_after, pair_features_after)
```

```python
import jax
import jax.numpy as jnp
import numpy as np
from jax import lax
from jax.experimental import pallas as pl
from jax.experimental.pallas import tpu as pltpu
from jax.sharding import PartitionSpec as P

HEAD_COUNT = 8
HEAD_CHANNELS = 32
OUTER_CHANNELS = 32
PAIR_DIM = 128


EPSILON = 1e-05
MASKED = -100000.0


def layer_norm(value_vectors, scale_vec, shift_vec):
    widened = value_vectors.astype(jnp.float32)
    centred = widened - jnp.mean(widened, axis=-1, keepdims=True)
    variance = jnp.mean(centred * centred, axis=-1, keepdims=True)
    scaled = centred * lax.rsqrt(variance + EPSILON)
    return (scaled * scale_vec + shift_vec).astype(jnp.bfloat16)


def heed_across_lanes(
    vertical_pieces,
    present_mask,
    focus_normal_factor,
    focus_normal_addend,
    probe_index_weights,
    payload_valve_weights,
    logistic_valve_addend,
    focus_exit_weights,
    focus_exit_addend,
):
    seq_count, res_count, feature_width = vertical_pieces.shape
    inner_channel_width = HEAD_COUNT * HEAD_CHANNELS
    normed = layer_norm(vertical_pieces, focus_normal_factor, focus_normal_addend).reshape(
        seq_count * res_count, feature_width
    )
    query_key = jnp.dot(normed, probe_index_weights, preferred_element_type=jnp.float32)
    value_gate = jnp.dot(normed, payload_valve_weights, preferred_element_type=jnp.float32)
    head_shape = (seq_count, res_count, HEAD_COUNT, HEAD_CHANNELS)
    query_rows_all = (
        (query_key[:, :inner_channel_width] * HEAD_CHANNELS ** (-0.5))
        .astype(jnp.bfloat16)
        .reshape(head_shape)
    )
    key_rows = query_key[:, inner_channel_width:].astype(jnp.bfloat16).reshape(head_shape)
    value_rows = value_gate[:, :inner_channel_width].astype(jnp.bfloat16).reshape(head_shape)
    gating = jax.nn.sigmoid(value_gate[:, inner_channel_width:] + logistic_valve_addend)
    scores = jnp.einsum(
        "srhd,trhd->rhst", query_rows_all, key_rows, preferred_element_type=jnp.float32
    )
    allowed = jnp.transpose(present_mask > 0)[:, None, None, :]
    scores = jnp.where(allowed, scores, MASKED)
    exponent = jnp.exp(scores - jnp.max(scores, axis=-1, keepdims=True))
    weights = (exponent / jnp.sum(exponent, axis=-1, keepdims=True)).astype(jnp.bfloat16)
    attended = jnp.einsum(
        "rhst,trhd->srhd", weights, value_rows, preferred_element_type=jnp.float32
    )
    gated_rows = (attended.reshape(seq_count * res_count, inner_channel_width) * gating).astype(
        jnp.bfloat16
    )
    update = (
        jnp.dot(gated_rows, focus_exit_weights, preferred_element_type=jnp.float32)
        + focus_exit_addend
    )
    return (
        vertical_pieces.astype(jnp.float32) + update.reshape(seq_count, res_count, feature_width)
    ).astype(jnp.bfloat16)


def project_pairs(
    revised_tensor,
    present_mask,
    product_mean_layer_stretch,
    product_mean_layer_shift,
    twin_map_matrix,
    twin_map_shift,
):
    seq_count, res_count, feature_width = revised_tensor.shape
    normed = layer_norm(
        revised_tensor, product_mean_layer_stretch, product_mean_layer_shift
    ).reshape(seq_count * res_count, feature_width)
    projected = (
        jnp.dot(normed, twin_map_matrix, preferred_element_type=jnp.float32) + twin_map_shift
    )
    projected = projected.reshape(seq_count, res_count, 2 * OUTER_CHANNELS) * present_mask[
        :, :, None
    ].astype(jnp.float32)
    projected = projected.astype(jnp.bfloat16)
    return (projected[:, :, :OUTER_CHANNELS], projected[:, :, OUTER_CHANNELS:])


def pair_tile(left_rows, right_cols, live_rows, live_cols, couple_map_matrix, couple_map_shift):
    row_count = left_rows.shape[1]
    col_count = right_cols.shape[1]
    outer_sum = jnp.einsum(
        "sic,sje->ijce", left_rows, right_cols, preferred_element_type=jnp.float32
    )
    counts = jnp.einsum("si,sj->ij", live_rows, live_cols, preferred_element_type=jnp.float32)
    mean_terms = (
        outer_sum.reshape(row_count, col_count, OUTER_CHANNELS * OUTER_CHANNELS)
        / jnp.maximum(counts, 1.0)[:, :, None]
    ).astype(jnp.bfloat16)
    result = jnp.dot(
        mean_terms.reshape(row_count * col_count, OUTER_CHANNELS * OUTER_CHANNELS),
        couple_map_matrix,
        preferred_element_type=jnp.float32,
    )
    result = result + couple_map_shift
    return result.astype(jnp.bfloat16).reshape(row_count, col_count, PAIR_DIM)


def tiled_pairs(left_rows, right_cols, live_rows, live_cols, couple_map_matrix, couple_map_shift):
    return pair_tile(
        left_rows, right_cols, live_rows, live_cols, couple_map_matrix, couple_map_shift
    )


def shards(
    homolog_stack_tensor,
    occupancy_indicator,
    chain_existence_flags,
    focus_normal_factor,
    focus_normal_addend,
    probe_index_weights,
    payload_valve_weights,
    logistic_valve_addend,
    focus_exit_weights,
    focus_exit_addend,
    product_mean_layer_stretch,
    product_mean_layer_shift,
    twin_map_matrix,
    twin_map_shift,
    couple_map_matrix,
    couple_map_shift,
):
    vertical_pieces = lax.all_to_all(
        homolog_stack_tensor, "dap", split_axis=1, concat_axis=0, tiled=True
    )
    seq_count, res_local, feature_width = vertical_pieces.shape
    position = lax.axis_index("dap")
    present_integer = occupancy_indicator * chain_existence_flags[:, None]
    live_all = present_integer.astype(jnp.bfloat16)
    live_own = lax.dynamic_slice_in_dim(present_integer, position * res_local, res_local, 1)
    revised_tensor = heed_across_lanes(
        vertical_pieces,
        live_own,
        focus_normal_factor,
        focus_normal_addend,
        probe_index_weights,
        payload_valve_weights,
        logistic_valve_addend,
        focus_exit_weights,
        focus_exit_addend,
    )
    left_own, right_own = project_pairs(
        revised_tensor,
        live_own,
        product_mean_layer_stretch,
        product_mean_layer_shift,
        twin_map_matrix,
        twin_map_shift,
    )
    live_rows = live_own.astype(jnp.bfloat16)
    pair_rows = tiled_pairs(
        left_own,
        lax.all_gather(right_own, "dap", axis=1, tiled=True),
        live_rows,
        live_all,
        couple_map_matrix,
        couple_map_shift,
    )
    return (revised_tensor, pair_rows)


FUSED_ROWS = 128


def normalise(rows, scale_row, shift_row):
    centred = rows - jnp.mean(rows, axis=-1, keepdims=True)
    variance = jnp.mean(centred * centred, axis=-1, keepdims=True)
    return (centred * lax.rsqrt(variance + EPSILON) * scale_row + shift_row).astype(jnp.bfloat16)


def column_kernel(
    x_ref,
    order_ref,
    live_ref,
    factor_ref,
    addend_ref,
    probe_ref,
    valve_ref,
    valve_addend_ref,
    exit_ref,
    exit_addend_ref,
    stretch_ref,
    shift_ref,
    twin_ref,
    twin_shift_ref,
    expand_ref,
    sum_ref,
    revised_ref,
    left_ref,
    right_ref,
    *,
    seq_count,
):
    rows, width = x_ref.shape
    inner = HEAD_COUNT * HEAD_CHANNELS
    f32 = jnp.float32
    bf16 = jnp.bfloat16
    x = jnp.dot(order_ref[...], x_ref[...], preferred_element_type=f32)
    normed = normalise(x, factor_ref[...], addend_ref[...])
    query_key = jnp.dot(normed, probe_ref[...], preferred_element_type=f32)
    value_gate = jnp.dot(normed, valve_ref[...], preferred_element_type=f32)
    query = (query_key[:, :inner] * HEAD_CHANNELS ** (-0.5)).astype(bf16)
    key = query_key[:, inner:].astype(bf16)
    value = value_gate[:, :inner].astype(bf16)
    gating = jax.nn.sigmoid(value_gate[:, inner:] + valve_addend_ref[...])
    lane = lax.broadcasted_iota(jnp.int32, (rows, inner), 1)
    zero = jnp.zeros((rows, inner), bf16)
    heads = [
        (lane >= h * HEAD_CHANNELS) & (lane < (h + 1) * HEAD_CHANNELS) for h in range(HEAD_COUNT)
    ]
    query_heads = jnp.concatenate([jnp.where(m, query, zero) for m in heads], axis=0)
    value_heads = jnp.concatenate([jnp.where(m, value, zero) for m in heads], axis=0)
    scores = lax.dot_general(
        query_heads, key, (((1,), (1,)), ((), ())), preferred_element_type=f32
    ).reshape(HEAD_COUNT, rows, rows)
    row_at = lax.broadcasted_iota(jnp.int32, (rows, rows), 0)
    col_at = lax.broadcasted_iota(jnp.int32, (rows, rows), 1)
    same = None
    for r in range(rows // seq_count):
        low, high = r * seq_count, (r + 1) * seq_count
        block = (row_at >= low) & (row_at < high) & (col_at >= low) & (col_at < high)
        same = block if same is None else same | block
    live = jnp.broadcast_to(live_ref[...], (rows, rows))
    allowed = same & (live > 0.0)
    other = jnp.where(same, MASKED, -jnp.inf)
    scores = jnp.where(allowed[None], scores, other[None])
    exponent = jnp.exp(scores - jnp.max(scores, axis=-1, keepdims=True))
    weights = (exponent / jnp.sum(exponent, axis=-1, keepdims=True)).astype(bf16)
    weights = jnp.concatenate([weights[h] for h in range(HEAD_COUNT)], axis=1)
    attended = jnp.dot(weights, value_heads, preferred_element_type=f32)
    gated = (attended * gating).astype(bf16)
    update = jnp.dot(gated, exit_ref[...], preferred_element_type=f32) + exit_addend_ref[...]
    revised = (x + update).astype(bf16)
    revised_ref[...] = revised
    normed = normalise(revised.astype(f32), stretch_ref[...], shift_ref[...])
    projected = lax.dot_general(
        normed, twin_ref[...], (((1,), (1,)), ((), ())), preferred_element_type=f32
    )
    live_col = jnp.sum(jnp.where(row_at == col_at, live, 0.0), axis=1, keepdims=True)
    projected = ((projected + twin_shift_ref[...]) * live_col).astype(bf16)
    left_ref[...] = projected[:, :OUTER_CHANNELS]
    spread = jnp.dot(projected, expand_ref[...], preferred_element_type=f32)
    wide = spread.shape[1]
    seq_row = lax.broadcasted_iota(jnp.int32, (rows, wide), 0) & (seq_count - 1)
    seq_col = lax.broadcasted_iota(jnp.int32, (rows, wide), 1) & (seq_count - 1)
    spread = jnp.where(seq_row == seq_col, spread, 0.0).astype(bf16)
    packed = jnp.dot(sum_ref[...], spread, preferred_element_type=f32)
    right_ref[...] = packed[: right_ref.shape[0]].astype(bf16)


def left_kernel(left_ref, couple_ref, out_ref, *, seq_count):
    rows = left_ref.shape[0]
    left = left_ref[...]
    for e in range(OUTER_CHANNELS):
        lanes = slice(e * PAIR_DIM, (e + 1) * PAIR_DIM)
        term = jnp.dot(left, couple_ref[:, lanes], preferred_element_type=jnp.float32)
        term = term.astype(jnp.bfloat16)
        for i in range(rows // seq_count):
            out_ref[e * seq_count : (e + 1) * seq_count, i * PAIR_DIM : (i + 1) * PAIR_DIM] = term[
                i * seq_count : (i + 1) * seq_count
            ]


def pair_kernel(right_ref, terms_ref, scale_ref, shift_ref, out_ref):
    result = jnp.dot(right_ref[...], terms_ref[...], preferred_element_type=jnp.float32)
    for i in range(out_ref.shape[0]):
        own = result[:, i * PAIR_DIM : (i + 1) * PAIR_DIM] * scale_ref[:, i : i + 1]
        out_ref[i] = (own + shift_ref[...]).astype(jnp.bfloat16)


def collect(block, axis_size, position):
    if axis_size & (axis_size - 1):
        return lax.all_gather(block, "dap", axis=0, tiled=True)
    step = 1
    while step < axis_size:
        pairs = [(j, j ^ step) for j in range(axis_size)]
        other = lax.ppermute(block, "dap", pairs)
        upper = (position & step) > 0
        block = jnp.where(
            upper,
            jnp.concatenate([other, block], axis=0),
            jnp.concatenate([block, other], axis=0),
        )
        step *= 2
    return block


def fused_shards(
    homolog_stack_tensor,
    occupancy_indicator,
    chain_existence_flags,
    focus_normal_factor,
    focus_normal_addend,
    probe_index_weights,
    payload_valve_weights,
    logistic_valve_addend,
    focus_exit_weights,
    focus_exit_addend,
    product_mean_layer_stretch,
    product_mean_layer_shift,
    twin_map_matrix,
    twin_map_shift,
    couple_map_matrix,
    couple_map_shift,
    axis_size,
):
    seq_local, res_count, width = homolog_stack_tensor.shape
    res_local = res_count // axis_size
    seq_count = seq_local * axis_size
    rows = seq_count * res_local
    bf16 = jnp.bfloat16
    sent = homolog_stack_tensor.reshape(seq_local, axis_size, res_local, width)
    sent = jnp.transpose(sent, (1, 2, 0, 3)).reshape(axis_size, res_local * seq_local, width)
    got = lax.all_to_all(sent, "dap", split_axis=0, concat_axis=0, tiled=True)
    got = got.reshape(rows, width)
    position = lax.axis_index("dap")
    present = occupancy_indicator * chain_existence_flags[:, None]
    live_own = lax.dynamic_slice_in_dim(present, position * res_local, res_local, 1)
    live_row = jnp.transpose(live_own).reshape(1, rows).astype(jnp.float32)
    counts = jnp.einsum(
        "sj,si->ji",
        present.astype(bf16),
        live_own.astype(bf16),
        preferred_element_type=jnp.float32,
    )
    scale = 1.0 / jnp.maximum(counts, 1.0)
    at = np.arange(rows)
    res_at, seq_at = at // seq_count, at % seq_count
    source = (seq_at // seq_local) * res_local * seq_local + res_at * seq_local + seq_at % seq_local
    order = jnp.asarray(source[:, None] == at[None, :], bf16)
    wide = OUTER_CHANNELS * seq_count
    expand = jnp.asarray(
        np.arange(2 * OUTER_CHANNELS)[:, None] == OUTER_CHANNELS + np.arange(wide)[None, :] // seq_count,
        bf16,
    )
    res_pad = -(-res_local // 8) * 8
    summing = jnp.asarray(np.arange(res_pad)[:, None] == res_at[None, :], bf16)
    as_row = lambda v: v.reshape(1, -1)
    vmem = pl.BlockSpec(memory_space=pltpu.VMEM)
    revised, left, right = pl.pallas_call(
        lambda *refs: column_kernel(*refs, seq_count=seq_count),
        out_shape=(
            jax.ShapeDtypeStruct((rows, width), bf16),
            jax.ShapeDtypeStruct((rows, OUTER_CHANNELS), bf16),
            jax.ShapeDtypeStruct((res_local, wide), bf16),
        ),
        in_specs=[vmem] * 16,
        out_specs=(vmem, vmem, vmem),
        name="column",
    )(
        got,
        order,
        live_row,
        as_row(focus_normal_factor),
        as_row(focus_normal_addend),
        probe_index_weights,
        payload_valve_weights,
        as_row(logistic_valve_addend),
        focus_exit_weights,
        as_row(focus_exit_addend),
        as_row(product_mean_layer_stretch),
        as_row(product_mean_layer_shift),
        jnp.transpose(twin_map_matrix),
        as_row(twin_map_shift),
        expand,
        summing,
    )
    terms = pl.pallas_call(
        lambda *refs: left_kernel(*refs, seq_count=seq_count),
        out_shape=jax.ShapeDtypeStruct((wide, res_local * PAIR_DIM), bf16),
        in_specs=[vmem] * 2,
        out_specs=vmem,
        cost_estimate=pl.CostEstimate(
            flops=4 * rows * OUTER_CHANNELS * OUTER_CHANNELS * PAIR_DIM,
            bytes_accessed=2 * wide * res_local * PAIR_DIM,
            transcendentals=0,
        ),
        name="terms",
    )(left, couple_map_matrix.reshape(OUTER_CHANNELS, OUTER_CHANNELS * PAIR_DIM))
    alignment_after = jnp.transpose(revised.reshape(res_local, seq_count, width), (1, 0, 2))
    right_all = collect(right, axis_size, position)
    pair_rows = pl.pallas_call(
        pair_kernel,
        out_shape=jax.ShapeDtypeStruct((res_local, res_count, PAIR_DIM), bf16),
        in_specs=[vmem] * 4,
        out_specs=vmem,
        name="pairs",
    )(right_all, terms, scale, as_row(couple_map_shift))
    return (alignment_after, pair_rows)


def solution(mesh):
    axis_size = mesh.shape["dap"]

    def step(*arrays):
        seq_local, res_count, _ = arrays[0].shape
        seq_count = seq_local * axis_size
        rows = seq_count * (res_count // axis_size)
        if rows <= FUSED_ROWS and seq_count & (seq_count - 1) == 0 and seq_count % 16 == 0:
            return fused_shards(*arrays, axis_size)
        return shards(*arrays)

    in_specs = (
        P(("grp", "dap"), None, None),
        P("grp", None),
        P("grp"),
        P(),
        P(),
        P(),
        P(),
        P(),
        P(),
        P(),
        P(),
        P(),
        P(),
        P(),
        P(),
        P(),
    )
    out_specs = (P("grp", "dap", None), P(("grp", "dap"), None, None))
    return jax.shard_map(step, mesh=mesh, in_specs=in_specs, out_specs=out_specs, check_vma=False)
```

```python
import jax
import jax.numpy as jnp
import numpy as np
from jax import lax
from jax.experimental import pallas as pl
from jax.experimental.pallas import tpu as pltpu
from jax.sharding import PartitionSpec as P

HEAD_COUNT = 8
HEAD_CHANNELS = 32
OUTER_CHANNELS = 32
PAIR_DIM = 128


EPSILON = 1e-05
MASKED = -100000.0


def layer_norm(value_vectors, scale_vec, shift_vec):
    widened = value_vectors.astype(jnp.float32)
    centred = widened - jnp.mean(widened, axis=-1, keepdims=True)
    variance = jnp.mean(centred * centred, axis=-1, keepdims=True)
    scaled = centred * lax.rsqrt(variance + EPSILON)
    return (scaled * scale_vec + shift_vec).astype(jnp.bfloat16)


def heed_across_lanes(
    vertical_pieces,
    present_mask,
    focus_normal_factor,
    focus_normal_addend,
    probe_index_weights,
    payload_valve_weights,
    logistic_valve_addend,
    focus_exit_weights,
    focus_exit_addend,
):
    seq_count, res_count, feature_width = vertical_pieces.shape
    inner_channel_width = HEAD_COUNT * HEAD_CHANNELS
    normed = layer_norm(vertical_pieces, focus_normal_factor, focus_normal_addend).reshape(
        seq_count * res_count, feature_width
    )
    query_key = jnp.dot(normed, probe_index_weights, preferred_element_type=jnp.float32)
    value_gate = jnp.dot(normed, payload_valve_weights, preferred_element_type=jnp.float32)
    head_shape = (seq_count, res_count, HEAD_COUNT, HEAD_CHANNELS)
    query_rows_all = (
        (query_key[:, :inner_channel_width] * HEAD_CHANNELS ** (-0.5))
        .astype(jnp.bfloat16)
        .reshape(head_shape)
    )
    key_rows = query_key[:, inner_channel_width:].astype(jnp.bfloat16).reshape(head_shape)
    value_rows = value_gate[:, :inner_channel_width].astype(jnp.bfloat16).reshape(head_shape)
    gating = jax.nn.sigmoid(value_gate[:, inner_channel_width:] + logistic_valve_addend)
    scores = jnp.einsum(
        "srhd,trhd->rhst", query_rows_all, key_rows, preferred_element_type=jnp.float32
    )
    allowed = jnp.transpose(present_mask > 0)[:, None, None, :]
    scores = jnp.where(allowed, scores, MASKED)
    exponent = jnp.exp(scores - jnp.max(scores, axis=-1, keepdims=True))
    weights = (exponent / jnp.sum(exponent, axis=-1, keepdims=True)).astype(jnp.bfloat16)
    attended = jnp.einsum(
        "rhst,trhd->srhd", weights, value_rows, preferred_element_type=jnp.float32
    )
    gated_rows = (attended.reshape(seq_count * res_count, inner_channel_width) * gating).astype(
        jnp.bfloat16
    )
    update = (
        jnp.dot(gated_rows, focus_exit_weights, preferred_element_type=jnp.float32)
        + focus_exit_addend
    )
    return (
        vertical_pieces.astype(jnp.float32) + update.reshape(seq_count, res_count, feature_width)
    ).astype(jnp.bfloat16)


def project_pairs(
    revised_tensor,
    present_mask,
    product_mean_layer_stretch,
    product_mean_layer_shift,
    twin_map_matrix,
    twin_map_shift,
):
    seq_count, res_count, feature_width = revised_tensor.shape
    normed = layer_norm(
        revised_tensor, product_mean_layer_stretch, product_mean_layer_shift
    ).reshape(seq_count * res_count, feature_width)
    projected = (
        jnp.dot(normed, twin_map_matrix, preferred_element_type=jnp.float32) + twin_map_shift
    )
    projected = projected.reshape(seq_count, res_count, 2 * OUTER_CHANNELS) * present_mask[
        :, :, None
    ].astype(jnp.float32)
    projected = projected.astype(jnp.bfloat16)
    return (projected[:, :, :OUTER_CHANNELS], projected[:, :, OUTER_CHANNELS:])


def pair_tile(left_rows, right_cols, live_rows, live_cols, couple_map_matrix, couple_map_shift):
    row_count = left_rows.shape[1]
    col_count = right_cols.shape[1]
    outer_sum = jnp.einsum(
        "sic,sje->ijce", left_rows, right_cols, preferred_element_type=jnp.float32
    )
    counts = jnp.einsum("si,sj->ij", live_rows, live_cols, preferred_element_type=jnp.float32)
    mean_terms = (
        outer_sum.reshape(row_count, col_count, OUTER_CHANNELS * OUTER_CHANNELS)
        / jnp.maximum(counts, 1.0)[:, :, None]
    ).astype(jnp.bfloat16)
    result = jnp.dot(
        mean_terms.reshape(row_count * col_count, OUTER_CHANNELS * OUTER_CHANNELS),
        couple_map_matrix,
        preferred_element_type=jnp.float32,
    )
    result = result + couple_map_shift
    return result.astype(jnp.bfloat16).reshape(row_count, col_count, PAIR_DIM)


def tiled_pairs(left_rows, right_cols, live_rows, live_cols, couple_map_matrix, couple_map_shift):
    return pair_tile(
        left_rows, right_cols, live_rows, live_cols, couple_map_matrix, couple_map_shift
    )


def shards(
    homolog_stack_tensor,
    occupancy_indicator,
    chain_existence_flags,
    focus_normal_factor,
    focus_normal_addend,
    probe_index_weights,
    payload_valve_weights,
    logistic_valve_addend,
    focus_exit_weights,
    focus_exit_addend,
    product_mean_layer_stretch,
    product_mean_layer_shift,
    twin_map_matrix,
    twin_map_shift,
    couple_map_matrix,
    couple_map_shift,
):
    vertical_pieces = lax.all_to_all(
        homolog_stack_tensor, "dap", split_axis=1, concat_axis=0, tiled=True
    )
    seq_count, res_local, feature_width = vertical_pieces.shape
    position = lax.axis_index("dap")
    present_integer = occupancy_indicator * chain_existence_flags[:, None]
    live_all = present_integer.astype(jnp.bfloat16)
    live_own = lax.dynamic_slice_in_dim(present_integer, position * res_local, res_local, 1)
    revised_tensor = heed_across_lanes(
        vertical_pieces,
        live_own,
        focus_normal_factor,
        focus_normal_addend,
        probe_index_weights,
        payload_valve_weights,
        logistic_valve_addend,
        focus_exit_weights,
        focus_exit_addend,
    )
    left_own, right_own = project_pairs(
        revised_tensor,
        live_own,
        product_mean_layer_stretch,
        product_mean_layer_shift,
        twin_map_matrix,
        twin_map_shift,
    )
    live_rows = live_own.astype(jnp.bfloat16)
    pair_rows = tiled_pairs(
        left_own,
        lax.all_gather(right_own, "dap", axis=1, tiled=True),
        live_rows,
        live_all,
        couple_map_matrix,
        couple_map_shift,
    )
    return (revised_tensor, pair_rows)


FUSED_ROWS = 128
SUBLANES = 8


def normalise(rows, scale_row, shift_row):
    centred = rows - jnp.mean(rows, axis=-1, keepdims=True)
    variance = jnp.mean(centred * centred, axis=-1, keepdims=True)
    return (centred * lax.rsqrt(variance + EPSILON) * scale_row + shift_row).astype(jnp.bfloat16)


def received_at(at, seq_count, seq_local, res_local):
    res_at, seq_at = at // seq_count, at % seq_count
    return (seq_at // seq_local * res_local + res_at) * seq_local + seq_at % seq_local


def sent_at(at, axis_size, seq_local, res_local):
    group, own = at // seq_local, at % seq_local
    return own * axis_size * res_local + group


def pack_kernel(x_ref, order_ref, out_ref):
    moved = jnp.dot(order_ref[...], x_ref[...], preferred_element_type=jnp.float32)
    out_ref[...] = moved.astype(jnp.bfloat16)


def column_kernel(
    x_ref,
    order_ref,
    live_ref,
    vectors_ref,
    probe_ref,
    valve_ref,
    exit_ref,
    twin_ref,
    expand_ref,
    revised_ref,
    left_ref,
    right_ref,
    *,
    seq_count,
):
    factor, addend, valve_addend, exit_addend, stretch, shift, twin_shift = (
        vectors_ref[k : k + 1, :] for k in range(7)
    )
    rows, width = x_ref.shape
    inner = HEAD_COUNT * HEAD_CHANNELS
    f32 = jnp.float32
    bf16 = jnp.bfloat16
    x = jnp.dot(order_ref[...], x_ref[...], preferred_element_type=f32)
    normed = normalise(x, factor, addend)
    query_key = jnp.dot(normed, probe_ref[...], preferred_element_type=f32)
    value_gate = jnp.dot(normed, valve_ref[...], preferred_element_type=f32)
    query = (query_key[:, :inner] * HEAD_CHANNELS ** (-0.5)).astype(bf16)
    key = query_key[:, inner:].astype(bf16)
    value = value_gate[:, :inner].astype(bf16)
    gating = jax.nn.sigmoid(value_gate[:, inner:] + valve_addend)
    lane = lax.broadcasted_iota(jnp.int32, (rows, inner), 1)
    zero = jnp.zeros((rows, inner), bf16)
    heads = [
        (lane >= h * HEAD_CHANNELS) & (lane < (h + 1) * HEAD_CHANNELS) for h in range(HEAD_COUNT)
    ]
    query_heads = jnp.concatenate([jnp.where(m, query, zero) for m in heads], axis=0)
    value_heads = jnp.concatenate([jnp.where(m, value, zero) for m in heads], axis=0)
    scores = lax.dot_general(
        query_heads, key, (((1,), (1,)), ((), ())), preferred_element_type=f32
    ).reshape(HEAD_COUNT, rows, rows)
    row_at = lax.broadcasted_iota(jnp.int32, (rows, rows), 0)
    col_at = lax.broadcasted_iota(jnp.int32, (rows, rows), 1)
    same = None
    for r in range(rows // seq_count):
        low, high = r * seq_count, (r + 1) * seq_count
        block = (row_at >= low) & (row_at < high) & (col_at >= low) & (col_at < high)
        same = block if same is None else same | block
    live = jnp.broadcast_to(live_ref[...], (rows, rows))
    allowed = same & (live > 0.0)
    other = jnp.where(same, MASKED, -jnp.inf)
    scores = jnp.where(allowed[None], scores, other[None])
    exponent = jnp.exp(scores - jnp.max(scores, axis=-1, keepdims=True))
    weights = (exponent / jnp.sum(exponent, axis=-1, keepdims=True)).astype(bf16)
    weights = jnp.concatenate([weights[h] for h in range(HEAD_COUNT)], axis=1)
    attended = jnp.dot(weights, value_heads, preferred_element_type=f32)
    gated = (attended * gating).astype(bf16)
    update = jnp.dot(gated, exit_ref[...], preferred_element_type=f32) + exit_addend
    revised = (x + update).astype(bf16)
    revised_ref[...] = revised
    normed = normalise(revised.astype(f32), stretch, shift)
    projected = lax.dot_general(
        normed, twin_ref[...], (((1,), (1,)), ((), ())), preferred_element_type=f32
    )
    live_col = jnp.sum(jnp.where(row_at == col_at, live, 0.0), axis=1, keepdims=True)
    projected = ((projected + twin_shift[:, : 2 * OUTER_CHANNELS]) * live_col).astype(bf16)
    left_ref[...] = projected[:, :OUTER_CHANNELS]
    spread = jnp.dot(projected, expand_ref[...], preferred_element_type=f32)
    wide = spread.shape[1]
    seq_row = lax.broadcasted_iota(jnp.int32, (rows, wide), 0) & (seq_count - 1)
    seq_col = lax.broadcasted_iota(jnp.int32, (rows, wide), 1) & (seq_count - 1)
    spread = jnp.where(seq_row == seq_col, spread, 0.0).astype(bf16)
    part_row = lax.broadcasted_iota(jnp.int32, (SUBLANES, rows), 0) * seq_count
    part_col = lax.broadcasted_iota(jnp.int32, (SUBLANES, rows), 1)
    parts = (part_col >= part_row) & (part_col < part_row + seq_count)
    packed = jnp.dot(parts.astype(bf16), spread, preferred_element_type=f32)
    right_ref[...] = packed[: right_ref.shape[0]].astype(bf16)


def left_kernel(left_ref, couple_ref, out_ref, *, seq_count):
    rows = left_ref.shape[0]
    left = left_ref[...]
    for e in range(OUTER_CHANNELS):
        lanes = slice(e * PAIR_DIM, (e + 1) * PAIR_DIM)
        term = jnp.dot(left, couple_ref[:, lanes], preferred_element_type=jnp.float32)
        term = term.astype(jnp.bfloat16)
        for i in range(rows // seq_count):
            out_ref[e * seq_count : (e + 1) * seq_count, i * PAIR_DIM : (i + 1) * PAIR_DIM] = term[
                i * seq_count : (i + 1) * seq_count
            ]


def pair_kernel(right_ref, terms_ref, scale_ref, vectors_ref, out_ref):
    shift = vectors_ref[7:8, :PAIR_DIM]
    result = jnp.dot(right_ref[...], terms_ref[...], preferred_element_type=jnp.float32)
    for i in range(out_ref.shape[0]):
        own = result[:, i * PAIR_DIM : (i + 1) * PAIR_DIM] * scale_ref[:, i : i + 1]
        out_ref[i] = (own + shift).astype(jnp.bfloat16)


def held(*arrays):
    return [pltpu.with_memory_space_constraint(a, pltpu.VMEM) for a in arrays]


def collect(block, axis_size, position, beside):
    if axis_size & (axis_size - 1):
        return lax.all_gather(block, "dap", axis=0, tiled=True), beside
    beside = list(beside)
    step = 1
    while step < axis_size:
        due = len(beside) - (axis_size // step).bit_length() + 1
        if 0 <= due < len(beside):
            block, beside[due] = lax.optimization_barrier((block, beside[due]))
        pairs = [(j, j ^ step) for j in range(axis_size)]
        other = lax.ppermute(block, "dap", pairs)
        upper = (position & step) > 0
        block = jnp.where(
            upper,
            jnp.concatenate([other, block], axis=0),
            jnp.concatenate([block, other], axis=0),
        )
        step *= 2
    return block, beside


def fused_shards(
    homolog_stack_tensor,
    occupancy_indicator,
    chain_existence_flags,
    focus_normal_factor,
    focus_normal_addend,
    probe_index_weights,
    payload_valve_weights,
    logistic_valve_addend,
    focus_exit_weights,
    focus_exit_addend,
    product_mean_layer_stretch,
    product_mean_layer_shift,
    twin_map_matrix,
    twin_map_shift,
    couple_map_matrix,
    couple_map_shift,
    axis_size,
):
    seq_local, res_count, width = homolog_stack_tensor.shape
    res_local = res_count // axis_size
    seq_count = seq_local * axis_size
    rows = seq_count * res_local
    bf16 = jnp.bfloat16
    vmem = pl.BlockSpec(memory_space=pltpu.VMEM)
    at = np.arange(rows)
    pack_order = jnp.asarray(
        sent_at(at, axis_size, seq_local, res_local)[:, None] == at[None, :], bf16
    )
    sent = pl.pallas_call(
        pack_kernel,
        out_shape=pltpu.VMEM((rows, width), bf16),
        in_specs=[vmem] * 2,
        out_specs=vmem,
        name="pack",
    )(homolog_stack_tensor.reshape(rows, width), pack_order)
    sent = sent.reshape(axis_size, res_local * seq_local, width)
    got = lax.all_to_all(sent, "dap", split_axis=0, concat_axis=0, tiled=True)
    got = got.reshape(rows, width)
    position = lax.axis_index("dap")
    present = occupancy_indicator * chain_existence_flags[:, None]
    live_own = lax.dynamic_slice_in_dim(present, position * res_local, res_local, 1)
    live_row = jnp.transpose(live_own).reshape(1, rows).astype(jnp.float32)
    counts = jnp.einsum(
        "sj,si->ji",
        present.astype(bf16),
        live_own.astype(bf16),
        preferred_element_type=jnp.float32,
    )
    scale = 1.0 / jnp.maximum(counts, 1.0)
    couple = couple_map_matrix.reshape(OUTER_CHANNELS, OUTER_CHANNELS * PAIR_DIM)
    as_row = lambda v: jnp.pad(v.reshape(1, -1), ((0, 0), (0, width - v.shape[0])))
    vectors = jnp.concatenate(
        [
            as_row(v)
            for v in (
                focus_normal_factor,
                focus_normal_addend,
                logistic_valve_addend,
                focus_exit_addend,
                product_mean_layer_stretch,
                product_mean_layer_shift,
                twin_map_shift,
                couple_map_shift,
            )
        ]
    )
    got, live_row, scale, couple, vectors = lax.optimization_barrier(
        (got, live_row, scale, couple, vectors)
    )
    order = jnp.asarray(
        received_at(at, seq_count, seq_local, res_local)[:, None] == at[None, :], bf16
    )
    wide = OUTER_CHANNELS * seq_count
    expand = jnp.asarray(
        np.arange(2 * OUTER_CHANNELS)[:, None] == OUTER_CHANNELS + np.arange(wide)[None, :] // seq_count,
        bf16,
    )
    revised, left, right = pl.pallas_call(
        lambda *refs: column_kernel(*refs, seq_count=seq_count),
        out_shape=(
            pltpu.VMEM((rows, width), bf16),
            pltpu.VMEM((rows, OUTER_CHANNELS), bf16),
            pltpu.VMEM((res_local, wide), bf16),
        ),
        in_specs=[vmem] * 9,
        out_specs=(vmem, vmem, vmem),
        name="column",
    )(
      *held(
        got,
        order,
        live_row,
        vectors,
        probe_index_weights,
        payload_valve_weights,
        focus_exit_weights,
        jnp.transpose(twin_map_matrix),
        expand,
      )
    )
    terms = pl.pallas_call(
        lambda *refs: left_kernel(*refs, seq_count=seq_count),
        out_shape=pltpu.VMEM((wide, res_local * PAIR_DIM), bf16),
        in_specs=[vmem] * 2,
        out_specs=vmem,
        cost_estimate=pl.CostEstimate(
            flops=4 * rows * OUTER_CHANNELS * OUTER_CHANNELS * PAIR_DIM,
            bytes_accessed=2 * wide * res_local * PAIR_DIM,
            transcendentals=0,
        ),
        name="terms",
    )(*held(left, couple))
    alignment_after = jnp.transpose(revised.reshape(res_local, seq_count, width), (1, 0, 2))
    right_all, (alignment_after, terms) = collect(
        right, axis_size, position, (alignment_after, terms)
    )
    pair_rows = pl.pallas_call(
        pair_kernel,
        out_shape=jax.ShapeDtypeStruct((res_local, res_count, PAIR_DIM), bf16),
        in_specs=[vmem] * 4,
        out_specs=vmem,
        name="pairs",
    )(*held(right_all, terms, scale, vectors))
    return (alignment_after, pair_rows)


def solution(mesh):
    axis_size = mesh.shape["dap"]

    def step(*arrays):
        seq_local, res_count, _ = arrays[0].shape
        seq_count = seq_local * axis_size
        rows = seq_count * (res_count // axis_size)
        if rows <= FUSED_ROWS and seq_count & (seq_count - 1) == 0 and seq_count % 16 == 0:
            return fused_shards(*arrays, axis_size)
        return shards(*arrays)

    in_specs = (
        P(("grp", "dap"), None, None),
        P("grp", None),
        P("grp"),
        P(),
        P(),
        P(),
        P(),
        P(),
        P(),
        P(),
        P(),
        P(),
        P(),
        P(),
        P(),
        P(),
    )
    out_specs = (P("grp", "dap", None), P(("grp", "dap"), None, None))
    return jax.shard_map(step, mesh=mesh, in_specs=in_specs, out_specs=out_specs, check_vma=False)
```

```python
import jax
import jax.numpy as jnp
import numpy as np
from jax import lax
from jax.experimental import pallas as pl
from jax.experimental.pallas import tpu as pltpu
from jax.sharding import PartitionSpec as P

HEAD_COUNT = 8
HEAD_CHANNELS = 32
OUTER_CHANNELS = 32
PAIR_DIM = 128


EPSILON = 1e-05
MASKED = -100000.0


def layer_norm(value_vectors, scale_vec, shift_vec):
    widened = value_vectors.astype(jnp.float32)
    centred = widened - jnp.mean(widened, axis=-1, keepdims=True)
    variance = jnp.mean(centred * centred, axis=-1, keepdims=True)
    scaled = centred * lax.rsqrt(variance + EPSILON)
    return (scaled * scale_vec + shift_vec).astype(jnp.bfloat16)


def heed_across_lanes(
    vertical_pieces,
    present_mask,
    focus_normal_factor,
    focus_normal_addend,
    probe_index_weights,
    payload_valve_weights,
    logistic_valve_addend,
    focus_exit_weights,
    focus_exit_addend,
):
    seq_count, res_count, feature_width = vertical_pieces.shape
    inner_channel_width = HEAD_COUNT * HEAD_CHANNELS
    normed = layer_norm(vertical_pieces, focus_normal_factor, focus_normal_addend).reshape(
        seq_count * res_count, feature_width
    )
    query_key = jnp.dot(normed, probe_index_weights, preferred_element_type=jnp.float32)
    value_gate = jnp.dot(normed, payload_valve_weights, preferred_element_type=jnp.float32)
    head_shape = (seq_count, res_count, HEAD_COUNT, HEAD_CHANNELS)
    query_rows_all = (
        (query_key[:, :inner_channel_width] * HEAD_CHANNELS ** (-0.5))
        .astype(jnp.bfloat16)
        .reshape(head_shape)
    )
    key_rows = query_key[:, inner_channel_width:].astype(jnp.bfloat16).reshape(head_shape)
    value_rows = value_gate[:, :inner_channel_width].astype(jnp.bfloat16).reshape(head_shape)
    gating = jax.nn.sigmoid(value_gate[:, inner_channel_width:] + logistic_valve_addend)
    scores = jnp.einsum(
        "srhd,trhd->rhst", query_rows_all, key_rows, preferred_element_type=jnp.float32
    )
    allowed = jnp.transpose(present_mask > 0)[:, None, None, :]
    scores = jnp.where(allowed, scores, MASKED)
    exponent = jnp.exp(scores - jnp.max(scores, axis=-1, keepdims=True))
    weights = (exponent / jnp.sum(exponent, axis=-1, keepdims=True)).astype(jnp.bfloat16)
    attended = jnp.einsum(
        "rhst,trhd->srhd", weights, value_rows, preferred_element_type=jnp.float32
    )
    gated_rows = (attended.reshape(seq_count * res_count, inner_channel_width) * gating).astype(
        jnp.bfloat16
    )
    update = (
        jnp.dot(gated_rows, focus_exit_weights, preferred_element_type=jnp.float32)
        + focus_exit_addend
    )
    return (
        vertical_pieces.astype(jnp.float32) + update.reshape(seq_count, res_count, feature_width)
    ).astype(jnp.bfloat16)


def project_pairs(
    revised_tensor,
    present_mask,
    product_mean_layer_stretch,
    product_mean_layer_shift,
    twin_map_matrix,
    twin_map_shift,
):
    seq_count, res_count, feature_width = revised_tensor.shape
    normed = layer_norm(
        revised_tensor, product_mean_layer_stretch, product_mean_layer_shift
    ).reshape(seq_count * res_count, feature_width)
    projected = (
        jnp.dot(normed, twin_map_matrix, preferred_element_type=jnp.float32) + twin_map_shift
    )
    projected = projected.reshape(seq_count, res_count, 2 * OUTER_CHANNELS) * present_mask[
        :, :, None
    ].astype(jnp.float32)
    projected = projected.astype(jnp.bfloat16)
    return (projected[:, :, :OUTER_CHANNELS], projected[:, :, OUTER_CHANNELS:])


def pair_tile(left_rows, right_cols, live_rows, live_cols, couple_map_matrix, couple_map_shift):
    row_count = left_rows.shape[1]
    col_count = right_cols.shape[1]
    outer_sum = jnp.einsum(
        "sic,sje->ijce", left_rows, right_cols, preferred_element_type=jnp.float32
    )
    counts = jnp.einsum("si,sj->ij", live_rows, live_cols, preferred_element_type=jnp.float32)
    mean_terms = (
        outer_sum.reshape(row_count, col_count, OUTER_CHANNELS * OUTER_CHANNELS)
        / jnp.maximum(counts, 1.0)[:, :, None]
    ).astype(jnp.bfloat16)
    result = jnp.dot(
        mean_terms.reshape(row_count * col_count, OUTER_CHANNELS * OUTER_CHANNELS),
        couple_map_matrix,
        preferred_element_type=jnp.float32,
    )
    result = result + couple_map_shift
    return result.astype(jnp.bfloat16).reshape(row_count, col_count, PAIR_DIM)


def tiled_pairs(left_rows, right_cols, live_rows, live_cols, couple_map_matrix, couple_map_shift):
    return pair_tile(
        left_rows, right_cols, live_rows, live_cols, couple_map_matrix, couple_map_shift
    )


def shards(
    homolog_stack_tensor,
    occupancy_indicator,
    chain_existence_flags,
    focus_normal_factor,
    focus_normal_addend,
    probe_index_weights,
    payload_valve_weights,
    logistic_valve_addend,
    focus_exit_weights,
    focus_exit_addend,
    product_mean_layer_stretch,
    product_mean_layer_shift,
    twin_map_matrix,
    twin_map_shift,
    couple_map_matrix,
    couple_map_shift,
):
    vertical_pieces = lax.all_to_all(
        homolog_stack_tensor, "dap", split_axis=1, concat_axis=0, tiled=True
    )
    seq_count, res_local, feature_width = vertical_pieces.shape
    position = lax.axis_index("dap")
    present_integer = occupancy_indicator * chain_existence_flags[:, None]
    live_all = present_integer.astype(jnp.bfloat16)
    live_own = lax.dynamic_slice_in_dim(present_integer, position * res_local, res_local, 1)
    revised_tensor = heed_across_lanes(
        vertical_pieces,
        live_own,
        focus_normal_factor,
        focus_normal_addend,
        probe_index_weights,
        payload_valve_weights,
        logistic_valve_addend,
        focus_exit_weights,
        focus_exit_addend,
    )
    left_own, right_own = project_pairs(
        revised_tensor,
        live_own,
        product_mean_layer_stretch,
        product_mean_layer_shift,
        twin_map_matrix,
        twin_map_shift,
    )
    live_rows = live_own.astype(jnp.bfloat16)
    pair_rows = tiled_pairs(
        left_own,
        lax.all_gather(right_own, "dap", axis=1, tiled=True),
        live_rows,
        live_all,
        couple_map_matrix,
        couple_map_shift,
    )
    return (revised_tensor, pair_rows)


FUSED_ROWS = 128
SUBLANES = 8


def normalise(rows, scale_row, shift_row):
    centred = rows - jnp.mean(rows, axis=-1, keepdims=True)
    variance = jnp.mean(centred * centred, axis=-1, keepdims=True)
    return (centred * lax.rsqrt(variance + EPSILON) * scale_row + shift_row).astype(jnp.bfloat16)


def received_at(at, seq_count, seq_local, res_local):
    res_at, seq_at = at // seq_count, at % seq_count
    return (seq_at // seq_local * res_local + res_at) * seq_local + seq_at % seq_local


def sent_at(at, axis_size, seq_local, res_local):
    group, own = at // seq_local, at % seq_local
    return own * axis_size * res_local + group


def pack_kernel(x_ref, order_ref, out_ref):
    moved = jnp.dot(order_ref[...], x_ref[...], preferred_element_type=jnp.float32)
    out_ref[...] = moved.astype(jnp.bfloat16)


def column_kernel(
    x_ref,
    order_ref,
    live_ref,
    vectors_ref,
    probe_ref,
    valve_ref,
    exit_ref,
    twin_ref,
    expand_ref,
    revised_ref,
    left_ref,
    right_ref,
    *,
    seq_count,
):
    factor, addend, valve_addend, exit_addend, stretch, shift, twin_shift = (
        vectors_ref[k : k + 1, :] for k in range(7)
    )
    rows, width = x_ref.shape
    inner = HEAD_COUNT * HEAD_CHANNELS
    f32 = jnp.float32
    bf16 = jnp.bfloat16
    x = jnp.dot(order_ref[...], x_ref[...], preferred_element_type=f32)
    normed = normalise(x, factor, addend)
    query_key = jnp.dot(normed, probe_ref[...], preferred_element_type=f32)
    value_gate = jnp.dot(normed, valve_ref[...], preferred_element_type=f32)
    query = (query_key[:, :inner] * HEAD_CHANNELS ** (-0.5)).astype(bf16)
    key = query_key[:, inner:].astype(bf16)
    value = value_gate[:, :inner].astype(bf16)
    gating = jax.nn.sigmoid(value_gate[:, inner:] + valve_addend)
    lane = lax.broadcasted_iota(jnp.int32, (rows, inner), 1)
    zero = jnp.zeros((rows, inner), bf16)
    heads = [
        (lane >= h * HEAD_CHANNELS) & (lane < (h + 1) * HEAD_CHANNELS) for h in range(HEAD_COUNT)
    ]
    query_heads = jnp.concatenate([jnp.where(m, query, zero) for m in heads], axis=0)
    value_heads = jnp.concatenate([jnp.where(m, value, zero) for m in heads], axis=0)
    scores = lax.dot_general(
        query_heads, key, (((1,), (1,)), ((), ())), preferred_element_type=f32
    ).reshape(HEAD_COUNT, rows, rows)
    row_at = lax.broadcasted_iota(jnp.int32, (rows, rows), 0)
    col_at = lax.broadcasted_iota(jnp.int32, (rows, rows), 1)
    same = None
    for r in range(rows // seq_count):
        low, high = r * seq_count, (r + 1) * seq_count
        block = (row_at >= low) & (row_at < high) & (col_at >= low) & (col_at < high)
        same = block if same is None else same | block
    live = jnp.broadcast_to(live_ref[...], (rows, rows))
    allowed = same & (live > 0.0)
    other = jnp.where(same, MASKED, -jnp.inf)
    scores = jnp.where(allowed[None], scores, other[None])
    exponent = jnp.exp(scores - jnp.max(scores, axis=-1, keepdims=True))
    weights = (exponent / jnp.sum(exponent, axis=-1, keepdims=True)).astype(bf16)
    weights = jnp.concatenate([weights[h] for h in range(HEAD_COUNT)], axis=1)
    attended = jnp.dot(weights, value_heads, preferred_element_type=f32)
    gated = (attended * gating).astype(bf16)
    update = jnp.dot(gated, exit_ref[...], preferred_element_type=f32) + exit_addend
    revised = (x + update).astype(bf16)
    revised_ref[...] = revised
    normed = normalise(revised.astype(f32), stretch, shift)
    projected = lax.dot_general(
        normed, twin_ref[...], (((1,), (1,)), ((), ())), preferred_element_type=f32
    )
    live_col = jnp.sum(jnp.where(row_at == col_at, live, 0.0), axis=1, keepdims=True)
    projected = ((projected + twin_shift[:, : 2 * OUTER_CHANNELS]) * live_col).astype(bf16)
    left_ref[...] = projected[:, :OUTER_CHANNELS]
    spread = jnp.dot(projected, expand_ref[...], preferred_element_type=f32)
    wide = spread.shape[1]
    seq_row = lax.broadcasted_iota(jnp.int32, (rows, wide), 0) & (seq_count - 1)
    seq_col = lax.broadcasted_iota(jnp.int32, (rows, wide), 1) & (seq_count - 1)
    spread = jnp.where(seq_row == seq_col, spread, 0.0).astype(bf16)
    part_row = lax.broadcasted_iota(jnp.int32, (SUBLANES, rows), 0) * seq_count
    part_col = lax.broadcasted_iota(jnp.int32, (SUBLANES, rows), 1)
    parts = (part_col >= part_row) & (part_col < part_row + seq_count)
    packed = jnp.dot(parts.astype(bf16), spread, preferred_element_type=f32)
    right_ref[...] = packed[: right_ref.shape[0]].astype(bf16)


def left_kernel(left_ref, couple_ref, out_ref, *, seq_count):
    rows = left_ref.shape[0]
    left = left_ref[...]
    for e in range(OUTER_CHANNELS):
        lanes = slice(e * PAIR_DIM, (e + 1) * PAIR_DIM)
        term = jnp.dot(left, couple_ref[:, lanes], preferred_element_type=jnp.float32)
        term = term.astype(jnp.bfloat16)
        for i in range(rows // seq_count):
            out_ref[e * seq_count : (e + 1) * seq_count, i * PAIR_DIM : (i + 1) * PAIR_DIM] = term[
                i * seq_count : (i + 1) * seq_count
            ]


def pair_kernel(right_ref, order_ref, terms_ref, scale_ref, vectors_ref, out_ref):
    shift = vectors_ref[7:8, :PAIR_DIM]
    right = jnp.dot(order_ref[...], right_ref[...], preferred_element_type=jnp.float32)
    right = right.astype(jnp.bfloat16)
    result = jnp.dot(right, terms_ref[...], preferred_element_type=jnp.float32)
    for i in range(out_ref.shape[0]):
        own = result[:, i * PAIR_DIM : (i + 1) * PAIR_DIM] * scale_ref[:, i : i + 1]
        out_ref[i] = (own + shift).astype(jnp.bfloat16)


def held(*arrays):
    return [pltpu.with_memory_space_constraint(a, pltpu.VMEM) for a in arrays]


def collect(block, axis_size, position, beside):
    if axis_size & (axis_size - 1):
        return lax.all_gather(block, "dap", axis=0, tiled=True), beside
    beside = list(beside)
    step, done = axis_size // 2, 0
    while step:
        if 0 < done <= len(beside):
            block, beside[done - 1] = lax.optimization_barrier((block, beside[done - 1]))
        pairs = [(j, j ^ step) for j in range(axis_size)]
        other = lax.ppermute(block, "dap", pairs)
        upper = (position & step) > 0
        block = jnp.where(
            upper,
            jnp.concatenate([other, block], axis=0),
            jnp.concatenate([block, other], axis=0),
        )
        step, done = step // 2, done + 1
    return block, beside


def collected_at(axis_size, part):
    if axis_size & (axis_size - 1):
        return np.arange(axis_size * part)
    order = np.zeros(1, np.int64)
    step = axis_size // 2
    while step:
        order = np.concatenate([order, order + step])
        step //= 2
    return (np.argsort(order)[:, None] * part + np.arange(part)).reshape(-1)


def fused_shards(
    homolog_stack_tensor,
    occupancy_indicator,
    chain_existence_flags,
    focus_normal_factor,
    focus_normal_addend,
    probe_index_weights,
    payload_valve_weights,
    logistic_valve_addend,
    focus_exit_weights,
    focus_exit_addend,
    product_mean_layer_stretch,
    product_mean_layer_shift,
    twin_map_matrix,
    twin_map_shift,
    couple_map_matrix,
    couple_map_shift,
    axis_size,
):
    seq_local, res_count, width = homolog_stack_tensor.shape
    res_local = res_count // axis_size
    seq_count = seq_local * axis_size
    rows = seq_count * res_local
    bf16 = jnp.bfloat16
    vmem = pl.BlockSpec(memory_space=pltpu.VMEM)
    at = np.arange(rows)
    pack_order = jnp.asarray(
        sent_at(at, axis_size, seq_local, res_local)[:, None] == at[None, :], bf16
    )
    sent = pl.pallas_call(
        pack_kernel,
        out_shape=pltpu.VMEM((rows, width), bf16),
        in_specs=[vmem] * 2,
        out_specs=vmem,
        name="pack",
    )(homolog_stack_tensor.reshape(rows, width), pack_order)
    sent = sent.reshape(axis_size, res_local * seq_local, width)
    got = lax.all_to_all(sent, "dap", split_axis=0, concat_axis=0, tiled=True)
    got = got.reshape(rows, width)
    position = lax.axis_index("dap")
    present = occupancy_indicator * chain_existence_flags[:, None]
    live_own = lax.dynamic_slice_in_dim(present, position * res_local, res_local, 1)
    live_row = jnp.transpose(live_own).reshape(1, rows).astype(jnp.float32)
    counts = jnp.einsum(
        "sj,si->ji",
        present.astype(bf16),
        live_own.astype(bf16),
        preferred_element_type=jnp.float32,
    )
    scale = 1.0 / jnp.maximum(counts, 1.0)
    couple = couple_map_matrix.reshape(OUTER_CHANNELS, OUTER_CHANNELS * PAIR_DIM)
    as_row = lambda v: jnp.pad(v.reshape(1, -1), ((0, 0), (0, width - v.shape[0])))
    vectors = jnp.concatenate(
        [
            as_row(v)
            for v in (
                focus_normal_factor,
                focus_normal_addend,
                logistic_valve_addend,
                focus_exit_addend,
                product_mean_layer_stretch,
                product_mean_layer_shift,
                twin_map_shift,
                couple_map_shift,
            )
        ]
    )
    got, live_row, scale, couple, vectors = lax.optimization_barrier(
        (got, live_row, scale, couple, vectors)
    )
    order = jnp.asarray(
        received_at(at, seq_count, seq_local, res_local)[:, None] == at[None, :], bf16
    )
    wide = OUTER_CHANNELS * seq_count
    expand = jnp.asarray(
        np.arange(2 * OUTER_CHANNELS)[:, None] == OUTER_CHANNELS + np.arange(wide)[None, :] // seq_count,
        bf16,
    )
    revised, left, right = pl.pallas_call(
        lambda *refs: column_kernel(*refs, seq_count=seq_count),
        out_shape=(
            pltpu.VMEM((rows, width), bf16),
            pltpu.VMEM((rows, OUTER_CHANNELS), bf16),
            pltpu.VMEM((res_local, wide), bf16),
        ),
        in_specs=[vmem] * 9,
        out_specs=(vmem, vmem, vmem),
        name="column",
    )(
      *held(
        got,
        order,
        live_row,
        vectors,
        probe_index_weights,
        payload_valve_weights,
        focus_exit_weights,
        jnp.transpose(twin_map_matrix),
        expand,
      )
    )
    terms = pl.pallas_call(
        lambda *refs: left_kernel(*refs, seq_count=seq_count),
        out_shape=pltpu.VMEM((wide, res_local * PAIR_DIM), bf16),
        in_specs=[vmem] * 2,
        out_specs=vmem,
        cost_estimate=pl.CostEstimate(
            flops=4 * rows * OUTER_CHANNELS * OUTER_CHANNELS * PAIR_DIM,
            bytes_accessed=2 * wide * res_local * PAIR_DIM,
            transcendentals=0,
        ),
        name="terms",
    )(*held(left, couple))
    alignment_after = jnp.transpose(revised.reshape(res_local, seq_count, width), (1, 0, 2))
    right_all, (alignment_after, terms) = collect(
        right, axis_size, position, (alignment_after, terms)
    )
    pair_order = jnp.asarray(
        collected_at(axis_size, res_local)[:, None] == np.arange(res_count)[None, :], bf16
    )
    pair_rows = pl.pallas_call(
        pair_kernel,
        out_shape=jax.ShapeDtypeStruct((res_local, res_count, PAIR_DIM), bf16),
        in_specs=[vmem] * 5,
        out_specs=vmem,
        name="pairs",
    )(*held(right_all, pair_order, terms, scale, vectors))
    return (alignment_after, pair_rows)


def solution(mesh):
    axis_size = mesh.shape["dap"]

    def step(*arrays):
        seq_local, res_count, _ = arrays[0].shape
        seq_count = seq_local * axis_size
        rows = seq_count * (res_count // axis_size)
        if rows <= FUSED_ROWS and seq_count & (seq_count - 1) == 0 and seq_count % 16 == 0:
            return fused_shards(*arrays, axis_size)
        return shards(*arrays)

    in_specs = (
        P(("grp", "dap"), None, None),
        P("grp", None),
        P("grp"),
        P(),
        P(),
        P(),
        P(),
        P(),
        P(),
        P(),
        P(),
        P(),
        P(),
        P(),
        P(),
        P(),
    )
    out_specs = (P("grp", "dap", None), P(("grp", "dap"), None, None))
    return jax.shard_map(step, mesh=mesh, in_specs=in_specs, out_specs=out_specs, check_vma=False)
```
